32 devices in a mesh: dp: 1 (over z), tp: 32 (over x, y, core).
Axes of the slice: x: 4, y: 4, z: 1, core: 2. Of those that a mesh axis runs over, the one named last changes fastest.
The devices are a block of a 4x4x8 slice.
Arguments:
- x: bfloat16 [2048, 8192], P('dp')
- w_gate: bfloat16 [8192, 32768], P(None, 'tp')
- w_up: bfloat16 [8192, 32768], P(None, 'tp')
- w_down: bfloat16 [32768, 8192], P('tp')
Outputs:
- output: bfloat16 [2048, 8192], P('dp')
All inputs are finite; a program needn't handle non-finite values.
Results may differ from the reference program's by a relative error of at most 0.016.
Values are sent between devices in bfloat16 or wider.
A program may use at most 768 MiB of HBM per device.

```python
import jax
import jax.numpy as jnp

ROWS = 2048
D = 8192
FF = 32768


def setup_inputs(seed: int = 0, part: int = 0) -> dict:
    kx, kg, ku, kd = jax.random.split(jax.random.key(seed), 4)
    drawn = {
        "x": jax.random.normal(jax.random.fold_in(kx, part), (ROWS, D), jnp.float32),
        "w_gate": jax.random.normal(kg, (D, FF), jnp.float32) * D**-0.5,
        "w_up": jax.random.normal(ku, (D, FF), jnp.float32) * D**-0.5,
        "w_down": jax.random.normal(kd, (FF, D), jnp.float32) * FF**-0.5,
    }
    return {k: v.astype(jnp.bfloat16) for k, v in drawn.items()}


def reference(x, w_gate, w_up, w_down):
    gate = jnp.dot(x, w_gate, preferred_element_type=jnp.float32)
    up = jnp.dot(x, w_up, preferred_element_type=jnp.float32)
    hidden = (jax.nn.silu(gate) * up).astype(jnp.bfloat16)
    return jnp.dot(hidden, w_down, preferred_element_type=jnp.float32).astype(jnp.bfloat16)
```

```python
import math

import jax
import jax.numpy as jnp
from jax import lax
from jax.experimental import pallas as pl
from jax.experimental.pallas import tpu as pltpu
from jax.sharding import PartitionSpec as P

MESH = pl.DeviceIdType.MESH
ROWS = 256
NT = 256
SIDE = 4
WD_SLOTS = 4
D_SLOTS = 3
STEPS = 12
POS = {
    "S1": [13, 25, 37, 49, 61, 74, 86, 97],
    "S2": [20, 32, 44, 56, 69, 81, 94, 101],
    "S3": [23, 35, 47, 60, 74, 86, 98, 105],
    "S4": [25, 39, 50, 62, 86, 94, 102, 108],
    "S5": [27, 45, 60, 69, 89, 99, 106, 111],
    "S6": [33, 49, 63, 74, 96, 103, 109, 113],
    "S7": [46, 60, 73, 85, 100, 107, 112, 115],
    "S8": [50, 70, 82, 94, 104, 110, 114, 116],
}
N_STEPS = 117
POS_BACK = 112


def _kernel(
    x_hbm, wg_hbm, wu_hbm, wd_hbm, y_hbm, wv,
    xv, hv, wd, acc, dsend, drecv,
    s1a, r1a, s1b, r1b, own, s2a, r2a, s2b, r2b, fin,
    x_sem, w_sem, wd_sem, d_ss, d_rs,
    s1a_ss, s1a_rs, s1b_ss, s1b_rs, s2a_ss, s2a_rs, s2b_ss, s2b_rs,
    fin_sem, g2a_ss, g2a_rs, g2b_ss, g2b_rs, g1a_ss, g1a_rs, g1b_ss, g1b_rs,
    dd_ss, dd_rs, credit, back_sem,
):
    chunks = x_hbm.shape[0] // ROWS
    cols = y_hbm.shape[1]
    half = cols // 2
    pc = half // SIDE
    nt = hv.shape[1] // NT
    first = chunks // 2
    up_rows = first * ROWS
    last = chunks - 1
    ph = ROWS // 2
    hp = ph // 2
    sr = ph // SIDE
    hs = sr // 2

    me = lax.axis_index("tp")
    core = lax.rem(me, 2)
    yi = lax.rem(me // 2, SIDE)
    xi = me // (2 * SIDE)

    def dev(a, b, c):
        return {"tp": (a * SIDE + b) * 2 + c}

    def mod(v):
        return lax.rem(v + 2 * SIDE, SIDE)

    partner = dev(xi, yi, 1 - core)
    x_nxt, x_prv = dev(mod(xi + 1), yi, core), dev(mod(xi - 1), yi, core)
    y_nxt, y_prv = dev(xi, mod(yi + 1), core), dev(xi, mod(yi - 1), core)
    me1, me2 = (xi, yi), (yi, xi)
    to1 = ((x_nxt, x_prv), (y_nxt, y_prv))
    to2 = ((y_nxt, y_prv), (x_nxt, x_prv))

    barrier = pltpu.get_barrier_semaphore()
    for d in (partner, x_nxt, x_prv, y_nxt, y_prv):
        pl.semaphore_signal(barrier, inc=1, device_id=d, device_id_type=MESH)

    def rcopy(src, dst, ss, rs, to):
        return pltpu.make_async_remote_copy(
            src_ref=src, dst_ref=dst, send_sem=ss, recv_sem=rs, device_id=to, device_id_type=MESH
        )

    def x_copy(t):
        return pltpu.make_async_copy(x_hbm.at[pl.ds(t * ROWS, ROWS), :], xv, x_sem)

    def w_tile(n, at, width):
        return wv.at[n // 2, :, pl.ds(pl.multiple_of((n % 2) * 2 * NT + at, NT), width)]

    def w_copies(n):
        c = pl.ds(n * NT, NT)
        return (
            pltpu.make_async_copy(wg_hbm.at[:, c], w_tile(n, 0, NT), w_sem.at[n, 0]),
            pltpu.make_async_copy(wu_hbm.at[:, c], w_tile(n, NT, NT), w_sem.at[n, 1]),
        )

    fx, fy = mod(xi + 2), mod(yi + 2)
    e = mod(fy - fx)
    o1 = jnp.maximum(e, 1)
    o2 = jnp.where(o1 == 1, 2, 1)
    o3 = jnp.where(o1 == 3, 2, 3)

    def piece_at(i):
        o = jnp.where(i == 0, 0, jnp.where(i == 1, o1, jnp.where(i == 2, o2, o3)))
        return mod(fx + o)

    def wd_copy(j):
        mine = j // SIDE
        hc = mine * core + (1 - mine) * (1 - core)
        c = pl.multiple_of(hc * half + piece_at(lax.rem(j, SIDE)) * pc, pc)
        s = lax.rem(j, WD_SLOTS)
        return pltpu.make_async_copy(wd_hbm.at[:, pl.ds(c, pc)], wd.at[s], wd_sem.at[s])

    x_copy(0).start()
    for n in range(nt):
        for c in w_copies(n):
            c.start()
    for j in range(WD_SLOTS):
        wd_copy(jnp.int32(j)).start()

    pl.semaphore_wait(barrier, 5)

    f32, bf16 = jnp.float32, jnp.bfloat16

    def gate_up(t, n):
        @pl.when(n == 0)
        def _():
            x_copy(t).wait()

        @pl.when(t == 0)
        def _():
            for c in w_copies(n):
                c.wait()

        for m in range(nt):
            @pl.when(n == m)
            def _():
                w = wv[m // 2, :, (m % 2) * 2 * NT : (m % 2 + 1) * 2 * NT]
                gu = jnp.dot(xv[...], w, preferred_element_type=f32)
                g, u = gu[:, :NT], gu[:, NT:]
                hv[:, m * NT : (m + 1) * NT] = (jax.nn.silu(g) * u).astype(bf16)

        @pl.when((n == nt - 1) & (t < last))
        def _():
            x_copy(t + 1).start()

        @pl.when((n == nt // 2 - 1) & (t == last))
        def _():
            for d in (partner, x_nxt, x_prv, y_nxt, y_prv):
                pl.semaphore_signal(credit, inc=1, device_id=d, device_id_type=MESH)

    def d_copy(t, q, n=0):
        s, m = lax.rem(t, 2), n % D_SLOTS
        return rcopy(dsend.at[m], drecv.at[s, q], d_ss.at[m], d_rs.at[s, q], partner)

    def down(t, j):
        s = lax.rem(j, WD_SLOTS)
        q = piece_at(lax.rem(j, SIDE))
        wd_copy(j).wait()

        @pl.when(j < SIDE)
        def _():
            n = t * SIDE + j

            @pl.when(n >= D_SLOTS)
            def _():
                d_copy(t, q, n).wait_send()

            r = jnp.dot(hv[...], wd[s], preferred_element_type=f32)
            dsend[lax.rem(n, D_SLOTS)] = r.astype(bf16)
            d_copy(t, q, n).start()

        @pl.when(j >= SIDE)
        def _():
            d_copy(t, q).wait_recv()
            r = jnp.dot(hv[...], wd[s], preferred_element_type=f32)
            acc[q] = r + drecv[lax.rem(t, 2), q].astype(f32)

        @pl.when(j < SIDE)
        def _():
            wd_copy(j + SIDE).start()

        @pl.when((j >= SIDE) & (t < last))
        def _():
            wd_copy(j - SIDE).start()

        @pl.when(j == SIDE + 1)
        def _():
            S0(t)

    hd = [(h, d) for h in range(2) for d in range(2)]

    def c1a(k, h, d):
        s = lax.rem(k, 2)
        return rcopy(s1a.at[h, d], r1a.at[s, h, d], s1a_ss.at[h, d], s1a_rs.at[s, h, d], to1[h][d])

    def c1b(k, h, d):
        s = lax.rem(k, 2)
        return rcopy(s1b.at[h, d], r1b.at[s, h, d], s1b_ss.at[h, d], s1b_rs.at[s, h, d], to1[h][d])

    def c2a(k, h, d):
        s = lax.rem(k, 2)
        return rcopy(s2a.at[h, d], r2a.at[s, h, d], s2a_ss.at[h, d], s2a_rs.at[s, h, d], to2[h][d])

    def c2b(k, h, d):
        s = lax.rem(k, 2)
        return rcopy(s2b.at[h, d], r2b.at[s, h, d], s2b_ss.at[h, d], s2b_rs.at[s, h, d], to2[h][d])

    def sent(copy, k, *a):
        @pl.when(k > 0)
        def _():
            copy(k - 1, *a).wait_send()

    def S0(k):
        s = lax.rem(k, 2)
        for h, d in hd:
            sent(c1a, k, h, d)
            far = mod(me1[h] + 2)
            s1a[h, d] = acc[far, pl.ds(h * ph + d * hp, hp), :].astype(bf16)
            c1a(k, h, d).start()

    def S1(k):
        s = lax.rem(k, 2)
        for h in range(2):
            own[s, h] = acc[me1[h], pl.ds(h * ph, ph), :]
        for h, d in hd:
            sent(c1b, k, h, d)
            c1a(k, h, d).wait_recv()
            near = mod(me1[h] + (1, -1)[d])
            other = 1 - d
            s1b[h, d, pl.ds(d * hp, hp), :] = (
                acc[near, pl.ds(h * ph + d * hp, hp), :] + r1a[s, h, d].astype(f32)
            ).astype(bf16)
            s1b[h, d, pl.ds(other * hp, hp), :] = acc[
                near, pl.ds(h * ph + other * hp, hp), :
            ].astype(bf16)
            c1b(k, h, d).start()

    def S2(k):
        s = lax.rem(k, 2)
        for h in range(2):
            for d in range(2):
                c1b(k, h, d).wait_recv()
            own[s, h] = (
                own[s, h]
                + r1b[s, h, 0].astype(f32)
                + r1b[s, h, 1].astype(f32)
            )
            far = mod(me2[h] + 2)
            for d in range(2):
                sent(c2a, k, h, d)
                r0 = pl.multiple_of(far * sr + d * hs, hs)
                s2a[h, d] = own[s, h, pl.ds(r0, hs), :].astype(bf16)
                c2a(k, h, d).start()

    def S3(k):
        s = lax.rem(k, 2)
        for h, d in hd:
            sent(c2b, k, h, d)
            c2a(k, h, d).wait_recv()
            near = mod(me2[h] + (1, -1)[d])
            other = 1 - d
            r0 = pl.multiple_of(near * sr + d * hs, hs)
            r1 = pl.multiple_of(near * sr + other * hs, hs)
            s2b[h, d, pl.ds(d * hs, hs), :] = (
                own[s, h, pl.ds(r0, hs), :] + r2a[s, h, d].astype(f32)
            ).astype(bf16)
            s2b[h, d, pl.ds(other * hs, hs), :] = own[s, h, pl.ds(r1, hs), :].astype(bf16)
            c2b(k, h, d).start()

    def region(k, vm, h, piece, r0, rows):
        p = core * SIDE + piece
        if vm:
            a = pl.multiple_of(p * up_rows + (k - first) * ROWS + h * ph + r0, 16)
            return wv.at[0, pl.ds(a, rows), :]
        a = pl.multiple_of(k * ROWS + h * ph + r0, 16)
        return y_hbm.at[pl.ds(a, rows), pl.ds(pl.multiple_of(p * pc, pc), pc)]

    def fin_local(k, h):
        s = lax.rem(k, 2)
        return pltpu.make_async_copy(
            fin.at[s, h], region(k, False, h, me1[h], me2[h] * sr, sr), fin_sem.at[s, h]
        )

    def g2a(k, vm, h, d):
        s = lax.rem(k, 2)
        return rcopy(
            fin.at[s, h], region(k, vm, h, me1[h], me2[h] * sr, sr),
            g2a_ss.at[s, h, d], g2a_rs.at[k, h, d], to2[h][d],
        )

    def g2b(k, vm, h, d):
        s = lax.rem(k, 2)
        src = mod(me2[h] - (1, -1)[d])
        r = region(k, vm, h, me1[h], src * sr + d * hs, hs)
        return rcopy(r, r, g2b_ss.at[s, h, d], g2b_rs.at[k, h, d], to2[h][d])

    def g1a(k, vm, h, d):
        s = lax.rem(k, 2)
        r = region(k, vm, h, me1[h], 0, ph)
        return rcopy(r, r, g1a_ss.at[s, h, d], g1a_rs.at[k, h, d], to1[h][d])

    def g1b(k, vm, h, d):
        s = lax.rem(k, 2)
        src = mod(me1[h] - (1, -1)[d])
        r = region(k, vm, h, src, d * hp, hp)
        return rcopy(r, r, g1b_ss.at[s, h, d], g1b_rs.at[k, h, d], to1[h][d])

    def dd(k, vm, h, o):
        s = lax.rem(k, 2)
        r = region(k, vm, h, mod(me1[h] + o), 0, ph)
        return rcopy(r, r, dd_ss.at[s, h, o], dd_rs.at[k, h, o], partner)

    def before(copy, k, vm, *a):
        @pl.when(k >= 2)
        def _():
            copy(k, vm, *a).wait_send()

    def S4(k, vm):
        s = lax.rem(k, 2)
        if vm:
            @pl.when(k == first)
            def _():
                pl.semaphore_wait(credit, 5)

        for h in range(2):
            for d in range(2):
                c2b(k, h, d).wait_recv()
                before(g2a, k, vm, h, d)
            r0 = pl.multiple_of(me2[h] * sr, sr)
            v = (
                own[s, h, pl.ds(r0, sr), :] + r2b[s, h, 0].astype(f32) + r2b[s, h, 1].astype(f32)
            ).astype(bf16)
            fin[s, h] = v
            if vm:
                a = pl.multiple_of(
                    (core * SIDE + me1[h]) * up_rows + (k - first) * ROWS + h * ph + me2[h] * sr, sr
                )
                wv[0, pl.ds(a, sr), :] = v
            for d in range(2):
                g2a(k, vm, h, d).start()
            if not vm:
                fin_local(k, h).start()

    def S5(k, vm):
        for h, d in hd:
            g2a(k, vm, h, d).wait_recv()
            before(g2b, k, vm, h, d)
            g2b(k, vm, h, d).start()
        if not vm:
            for h in range(2):
                fin_local(k, h).wait()

    def S6(k, vm):
        for h in range(2):
            for d in range(2):
                g2b(k, vm, h, d).wait_recv()
            for d in range(2):
                before(g1a, k, vm, h, d)
                g1a(k, vm, h, d).start()

    def S7(k, vm):
        for h, d in hd:
            g1a(k, vm, h, d).wait_recv()
            before(g1b, k, vm, h, d)
            g1b(k, vm, h, d).start()
        for h in range(2):
            for o in (0, 1, 3):
                before(dd, k, vm, h, o)
                dd(k, vm, h, o).start()

    def S8(k, vm):
        for h, d in hd:
            g1b(k, vm, h, d).wait_recv()
        for h in range(2):
            before(dd, k, vm, h, 2)
            dd(k, vm, h, 2).start()

    ho = [(h, o) for h in range(2) for o in range(4)]

    def back(p):
        return pltpu.make_async_copy(
            y_hbm.at[:, pl.ds(p * pc, pc)], wv.at[1, pl.ds(p * up_rows, up_rows), :], back_sem.at[p]
        )

    reduce = dict(S1=S1, S2=S2, S3=S3)
    gather = dict(S4=S4, S5=S5, S6=S6, S7=S7, S8=S8)

    @pl.loop(0, N_STEPS)
    def _(step):
        t, i = step // STEPS, lax.rem(step, STEPS)

        @pl.when((t < chunks) & (i < nt))
        def _():
            gate_up(t, i)

        @pl.when((t < chunks) & (i >= nt))
        def _():
            down(t, i - nt)

        for name in ("S2", "S4", "S1", "S3", "S5", "S6", "S7", "S8"):
            at = POS[name]
            assert len(at) == chunks
            hit = step == at[0]
            k = jnp.int32(0)
            for p in at[1:]:
                hit = hit | (step == p)
            for p in at:
                k = k + jnp.where(step > p, 1, 0)
            if name in reduce:
                @pl.when(hit)
                def _():
                    reduce[name](k)
            else:
                @pl.when(hit & (k < first))
                def _():
                    gather[name](k, False)

                @pl.when(hit & (k >= first))
                def _():
                    gather[name](k, True)

        @pl.when(step == POS_BACK)
        def _():
            @pl.loop(0, first)
            def _(k):
                for h, o in ho:
                    dd(k, False, h, o).wait_recv()

            for p in range(2 * SIDE):
                back(p).start()

    for p in range(2 * SIDE):
        back(p).wait()
    for k in range(first, chunks):
        for h, o in ho:
            dd(k, True, h, o).wait_recv()
    for n in range(D_SLOTS):
        d_copy(last, 0, n).wait_send()
    for f in (c1a, c1b, c2a, c2b):
        for h, d in hd:
            f(last, h, d).wait_send()
    for k in (last - 1, last):
        for f in (g2a, g2b, g1a, g1b):
            for h, d in hd:
                f(k, True, h, d).wait_send()
        for h, o in ho:
            dd(k, True, h, o).wait_send()


def _write(v_ref, y_ref, sem):
    pieces = y_ref.shape[1] // v_ref.shape[2]
    rows = v_ref.shape[1] // pieces
    copies = []
    for g in range(2):
        for p in range(pieces):
            src = v_ref.at[1 - g, pl.ds(p * rows, rows), :]
            dst = y_ref.at[pl.ds(g * rows, rows), pl.ds(p * v_ref.shape[2], v_ref.shape[2])]
            copies.append(pltpu.make_async_copy(src, dst, sem.at[g, p]))
    for c in copies:
        c.start()
    for c in copies:
        c.wait()


def solution(mesh):
    def step(x, w_gate, w_up, w_down):
        rows, depth = x.shape
        hidden = w_gate.shape[1]
        cols = w_down.shape[1]
        chunks = rows // ROWS
        pc = cols // 2 // SIDE
        ph = ROWS // 2
        sr = ph // SIDE
        assert mesh.shape["tp"] == 2 * SIDE * SIDE
        assert depth == cols and SIDE * rows == depth and hidden == 4 * NT == pc
        bf16, f32 = jnp.bfloat16, jnp.float32
        dma = pltpu.SemaphoreType.DMA
        V = pltpu.VMEM
        _, v = pl.pallas_call(
            _kernel,
            out_shape=(
                jax.ShapeDtypeStruct((rows // 2, cols), bf16),
                pltpu.VMEM((2, depth, pc), bf16),
            ),
            in_specs=[pl.BlockSpec(memory_space=pl.ANY)] * 4,
            out_specs=(
                pl.BlockSpec(memory_space=pl.ANY),
                pl.BlockSpec(memory_space=pltpu.VMEM),
            ),
            scratch_shapes=[
                V((ROWS, depth), bf16),
                V((ROWS, hidden), bf16),
                V((WD_SLOTS, hidden, pc), bf16),
                V((SIDE, ROWS, pc), f32),
                V((D_SLOTS, ROWS, pc), bf16),
                V((2, SIDE, ROWS, pc), bf16),
                V((2, 2, ph // 2, pc), bf16),
                V((2, 2, 2, ph // 2, pc), bf16),
                V((2, 2, ph, pc), bf16),
                V((2, 2, 2, ph, pc), bf16),
                V((2, 2, ph, pc), f32),
                V((2, 2, sr // 2, pc), bf16),
                V((2, 2, 2, sr // 2, pc), bf16),
                V((2, 2, sr, pc), bf16),
                V((2, 2, 2, sr, pc), bf16),
                V((2, 2, sr, pc), bf16),
                dma, dma((hidden // NT, 2)), dma((WD_SLOTS,)), dma((D_SLOTS,)), dma((2, SIDE)),
                dma((2, 2)), dma((2, 2, 2)), dma((2, 2)), dma((2, 2, 2)),
                dma((2, 2)), dma((2, 2, 2)), dma((2, 2)), dma((2, 2, 2)),
                dma((2, 2)),
                dma((2, 2, 2)), dma((chunks, 2, 2)), dma((2, 2, 2)), dma((chunks, 2, 2)),
                dma((2, 2, 2)), dma((chunks, 2, 2)), dma((2, 2, 2)), dma((chunks, 2, 2)),
                dma((2, 2, SIDE)), dma((chunks, 2, SIDE)),
                pltpu.SemaphoreType.REGULAR, dma((2 * SIDE,)),
            ],
            compiler_params=pltpu.CompilerParams(
                collective_id=0, has_side_effects=True, vmem_limit_bytes=67043328 - 4 * depth * pc
            ),
            cost_estimate=pl.CostEstimate(
                flops=6 * rows * depth * hidden, bytes_accessed=0, transcendentals=0
            ),
        )(x, w_gate, w_up, w_down)

        return pl.pallas_call(
            _write,
            out_shape=jax.ShapeDtypeStruct((rows, cols), bf16),
            in_specs=[pl.BlockSpec(memory_space=pltpu.VMEM)],
            out_specs=pl.BlockSpec(memory_space=pl.ANY),
            scratch_shapes=[dma((2, 2 * SIDE))],
            compiler_params=pltpu.CompilerParams(vmem_limit_bytes=2**22),
        )(pltpu.with_memory_space_constraint(v, pltpu.VMEM))

    return jax.shard_map(
        step,
        mesh=mesh,
        in_specs=(P("dp", None), P(None, "tp"), P(None, "tp"), P("tp", None)),
        out_specs=P("dp", None),
        check_vma=False,
    )
```

```python
import math

import jax
import jax.numpy as jnp
from jax import lax
from jax.experimental import pallas as pl
from jax.experimental.pallas import tpu as pltpu
from jax.sharding import PartitionSpec as P

MESH = pl.DeviceIdType.MESH
ROWS = 256
NT = 256
SIDE = 4
WD_SLOTS = 4
D_SLOTS = 3
STEPS = 12
POS = {
    "S1": [13, 25, 38, 52, 61, 72, 86, 101],
    "S2": [16, 28, 44, 58, 69, 78, 91, 104],
    "S3": [20, 34, 47, 61, 73, 84, 95, 106],
    "S4": [24, 38, 50, 66, 86, 87, 103, 116],
    "S5": [26, 41, 55, 71, 86, 101, 108, 120],
    "S6": [31, 49, 62, 74, 88, 104, 116, 123],
    "S7": [38, 53, 78, 80, 101, 114, 122, 131],
    "S8": [56, 79, 103, 104, 108, 118, 123, 131],
}
N_STEPS = 132
POS_BACK = 121


def _kernel(
    x_hbm, wg_hbm, wu_hbm, wd_hbm, y_hbm, wv,
    xv, hv, wd, acc, dsend, drecv,
    s1a, r1a, s1b, r1b, own, s2a, r2a, s2b, r2b, fin,
    x_sem, w_sem, wd_sem, d_ss, d_rs,
    s1a_ss, s1a_rs, s1b_ss, s1b_rs, s2a_ss, s2a_rs, s2b_ss, s2b_rs,
    fin_sem, g2a_ss, g2a_rs, g2b_ss, g2b_rs, g1a_ss, g1a_rs, g1b_ss, g1b_rs,
    dd_ss, dd_rs, credit, back_sem,
):
    chunks = x_hbm.shape[0] // ROWS
    cols = y_hbm.shape[1]
    half = cols // 2
    pc = half // SIDE
    nt = hv.shape[1] // NT
    first = chunks // 2
    up_rows = first * ROWS
    last = chunks - 1
    ph = ROWS // 2
    hp = ph // 2
    sr = ph // SIDE
    hs = sr // 2

    me = lax.axis_index("tp")
    core = lax.rem(me, 2)
    yi = lax.rem(me // 2, SIDE)
    xi = me // (2 * SIDE)

    def dev(a, b, c):
        return {"tp": (a * SIDE + b) * 2 + c}

    def mod(v):
        return lax.rem(v + 2 * SIDE, SIDE)

    partner = dev(xi, yi, 1 - core)
    x_nxt, x_prv = dev(mod(xi + 1), yi, core), dev(mod(xi - 1), yi, core)
    y_nxt, y_prv = dev(xi, mod(yi + 1), core), dev(xi, mod(yi - 1), core)
    me1, me2 = (xi, yi), (yi, xi)
    to1 = ((x_nxt, x_prv), (y_nxt, y_prv))
    to2 = ((y_nxt, y_prv), (x_nxt, x_prv))

    barrier = pltpu.get_barrier_semaphore()
    for d in (partner, x_nxt, x_prv, y_nxt, y_prv):
        pl.semaphore_signal(barrier, inc=1, device_id=d, device_id_type=MESH)

    def rcopy(src, dst, ss, rs, to):
        return pltpu.make_async_remote_copy(
            src_ref=src, dst_ref=dst, send_sem=ss, recv_sem=rs, device_id=to, device_id_type=MESH
        )

    def x_copy(t):
        return pltpu.make_async_copy(x_hbm.at[pl.ds(t * ROWS, ROWS), :], xv, x_sem)

    def w_tile(n, at, width):
        return wv.at[n // 2, :, pl.ds(pl.multiple_of((n % 2) * 2 * NT + at, NT), width)]

    def w_copies(n):
        c = pl.ds(n * NT, NT)
        return (
            pltpu.make_async_copy(wg_hbm.at[:, c], w_tile(n, 0, NT), w_sem.at[n, 0]),
            pltpu.make_async_copy(wu_hbm.at[:, c], w_tile(n, NT, NT), w_sem.at[n, 1]),
        )

    fx, fy = mod(xi + 2), mod(yi + 2)
    e = mod(fy - fx)
    o1 = jnp.maximum(e, 1)
    o2 = jnp.where(o1 == 1, 2, 1)
    o3 = jnp.where(o1 == 3, 2, 3)

    def piece_at(i):
        o = jnp.where(i == 0, 0, jnp.where(i == 1, o1, jnp.where(i == 2, o2, o3)))
        return mod(fx + o)

    def wd_copy(j):
        mine = j // SIDE
        hc = mine * core + (1 - mine) * (1 - core)
        c = pl.multiple_of(hc * half + piece_at(lax.rem(j, SIDE)) * pc, pc)
        s = lax.rem(j, WD_SLOTS)
        return pltpu.make_async_copy(wd_hbm.at[:, pl.ds(c, pc)], wd.at[s], wd_sem.at[s])

    x_copy(0).start()
    for n in range(nt):
        for c in w_copies(n):
            c.start()
    for j in range(WD_SLOTS):
        wd_copy(jnp.int32(j)).start()

    pl.semaphore_wait(barrier, 5)

    f32, bf16 = jnp.float32, jnp.bfloat16

    def gate_up(t, n):
        @pl.when(n == 0)
        def _():
            x_copy(t).wait()

        @pl.when(t == 0)
        def _():
            for c in w_copies(n):
                c.wait()

        for m in range(nt):
            @pl.when(n == m)
            def _():
                w = wv[m // 2, :, (m % 2) * 2 * NT : (m % 2 + 1) * 2 * NT]
                gu = jnp.dot(xv[...], w, preferred_element_type=f32)
                g, u = gu[:, :NT], gu[:, NT:]
                hv[:, m * NT : (m + 1) * NT] = (jax.nn.silu(g) * u).astype(bf16)

        @pl.when((n == nt - 1) & (t < last))
        def _():
            x_copy(t + 1).start()

        @pl.when((n == nt // 2 - 1) & (t == last))
        def _():
            for d in (partner, x_nxt, x_prv, y_nxt, y_prv):
                pl.semaphore_signal(credit, inc=1, device_id=d, device_id_type=MESH)

    def d_copy(t, q, n=0):
        s, m = lax.rem(t, 2), n % D_SLOTS
        return rcopy(dsend.at[m], drecv.at[s, q], d_ss.at[m], d_rs.at[s, q], partner)

    def down(t, j):
        s = lax.rem(j, WD_SLOTS)
        q = piece_at(lax.rem(j, SIDE))
        wd_copy(j).wait()

        @pl.when(j < SIDE)
        def _():
            n = t * SIDE + j

            @pl.when(n >= D_SLOTS)
            def _():
                d_copy(t, q, n).wait_send()

            r = jnp.dot(hv[...], wd[s], preferred_element_type=f32)
            dsend[lax.rem(n, D_SLOTS)] = r.astype(bf16)
            d_copy(t, q, n).start()

        @pl.when(j >= SIDE)
        def _():
            d_copy(t, q).wait_recv()
            r = jnp.dot(hv[...], wd[s], preferred_element_type=f32)
            acc[q] = r + drecv[lax.rem(t, 2), q].astype(f32)

        @pl.when(j < SIDE)
        def _():
            wd_copy(j + SIDE).start()

        @pl.when((j >= SIDE) & (t < last))
        def _():
            wd_copy(j - SIDE).start()

        @pl.when(j == SIDE + 1)
        def _():
            S0(t)

        @pl.when(j == 2 * SIDE - 1)
        def _():
            S0b(t)

    hd = [(h, d) for h in range(2) for d in range(2)]

    def c1a(k, h, d):
        s = lax.rem(k, 2)
        return rcopy(s1a.at[h, d], r1a.at[s, h, d], s1a_ss.at[h, d], s1a_rs.at[s, h, d], to1[h][d])

    def hrows(d, p):
        return pl.ds((d if p == 0 else 1 - d) * hp, hp)

    def c1b(k, h, d, p):
        s, r = lax.rem(k, 2), hrows(d, p)
        return rcopy(
            s1b.at[h, d, r, :], r1b.at[s, h, d, r, :],
            s1b_ss.at[h, d, p], s1b_rs.at[s, h, d, p], to1[h][d],
        )

    def c2a(k, h, d):
        s = lax.rem(k, 2)
        return rcopy(s2a.at[h, d], r2a.at[s, h, d], s2a_ss.at[h, d], s2a_rs.at[s, h, d], to2[h][d])

    def c2b(k, h, d):
        s = lax.rem(k, 2)
        return rcopy(s2b.at[h, d], r2b.at[s, h, d], s2b_ss.at[h, d], s2b_rs.at[s, h, d], to2[h][d])

    def sent(copy, k, *a):
        @pl.when(k > 0)
        def _():
            copy(k - 1, *a).wait_send()

    def S0(k):
        s = lax.rem(k, 2)
        for h, d in hd:
            sent(c1a, k, h, d)
            far = mod(me1[h] + 2)
            s1a[h, d] = acc[far, pl.ds(h * ph + d * hp, hp), :].astype(bf16)
            c1a(k, h, d).start()

    def S0b(k):
        for h, d in hd:
            sent(c1b, k, h, d, 1)
            near = mod(me1[h] + (1, -1)[d])
            s1b[h, d, hrows(d, 1), :] = acc[near, pl.ds(h * ph + (1 - d) * hp, hp), :].astype(bf16)
            c1b(k, h, d, 1).start()

    def S1(k):
        s = lax.rem(k, 2)
        for h, d in hd:
            sent(c1b, k, h, d, 0)
            c1a(k, h, d).wait_recv()
            near = mod(me1[h] + (1, -1)[d])
            s1b[h, d, hrows(d, 0), :] = (
                acc[near, pl.ds(h * ph + d * hp, hp), :] + r1a[s, h, d].astype(f32)
            ).astype(bf16)
            c1b(k, h, d, 0).start()
        for h in range(2):
            own[s, h] = acc[me1[h], pl.ds(h * ph, ph), :]

    def S2(k):
        s = lax.rem(k, 2)
        for h in range(2):
            for d in range(2):
                for p in range(2):
                    c1b(k, h, d, p).wait_recv()
            own[s, h] = (
                own[s, h]
                + r1b[s, h, 0].astype(f32)
                + r1b[s, h, 1].astype(f32)
            )
            far = mod(me2[h] + 2)
            for d in range(2):
                sent(c2a, k, h, d)
                r0 = pl.multiple_of(far * sr + d * hs, hs)
                s2a[h, d] = own[s, h, pl.ds(r0, hs), :].astype(bf16)
                c2a(k, h, d).start()

    def S3(k):
        s = lax.rem(k, 2)
        for h, d in hd:
            sent(c2b, k, h, d)
            c2a(k, h, d).wait_recv()
            near = mod(me2[h] + (1, -1)[d])
            other = 1 - d
            r0 = pl.multiple_of(near * sr + d * hs, hs)
            r1 = pl.multiple_of(near * sr + other * hs, hs)
            s2b[h, d, pl.ds(d * hs, hs), :] = (
                own[s, h, pl.ds(r0, hs), :] + r2a[s, h, d].astype(f32)
            ).astype(bf16)
            s2b[h, d, pl.ds(other * hs, hs), :] = own[s, h, pl.ds(r1, hs), :].astype(bf16)
            c2b(k, h, d).start()

    def region(k, vm, h, piece, r0, rows):
        p = core * SIDE + piece
        if vm:
            a = pl.multiple_of(p * up_rows + (k - first) * ROWS + h * ph + r0, 16)
            return wv.at[0, pl.ds(a, rows), :]
        a = pl.multiple_of(k * ROWS + h * ph + r0, 16)
        return y_hbm.at[pl.ds(a, rows), pl.ds(pl.multiple_of(p * pc, pc), pc)]

    def fin_local(k, h):
        s = lax.rem(k, 2)
        return pltpu.make_async_copy(
            fin.at[s, h], region(k, False, h, me1[h], me2[h] * sr, sr), fin_sem.at[s, h]
        )

    def g2a(k, vm, h, d):
        s = lax.rem(k, 2)
        return rcopy(
            fin.at[s, h], region(k, vm, h, me1[h], me2[h] * sr, sr),
            g2a_ss.at[s, h, d], g2a_rs.at[k, h, d], to2[h][d],
        )

    def g2b(k, vm, h, d):
        s = lax.rem(k, 2)
        src = mod(me2[h] - (1, -1)[d])
        r = region(k, vm, h, me1[h], src * sr + d * hs, hs)
        return rcopy(r, r, g2b_ss.at[s, h, d], g2b_rs.at[k, h, d], to2[h][d])

    def g1a(k, vm, h, d, p):
        s = lax.rem(k, 2)
        r = region(k, vm, h, me1[h], (d if p == 0 else 1 - d) * hp, hp)
        return rcopy(r, r, g1a_ss.at[s, h, d, p], g1a_rs.at[k, h, d, p], to1[h][d])

    def g1b(k, vm, h, d):
        s = lax.rem(k, 2)
        src = mod(me1[h] - (1, -1)[d])
        r = region(k, vm, h, src, d * hp, hp)
        return rcopy(r, r, g1b_ss.at[s, h, d], g1b_rs.at[k, h, d], to1[h][d])

    def dd(k, vm, h, o):
        s = lax.rem(k, 2)
        r = region(k, vm, h, mod(me1[h] + o), 0, ph)
        return rcopy(r, r, dd_ss.at[s, h, o], dd_rs.at[k, h, o], partner)

    def before(copy, k, vm, *a):
        @pl.when(k >= 2)
        def _():
            copy(k, vm, *a).wait_send()

    def S4(k, vm):
        s = lax.rem(k, 2)
        if vm:
            @pl.when(k == first)
            def _():
                pl.semaphore_wait(credit, 5)

        for h in range(2):
            for d in range(2):
                c2b(k, h, d).wait_recv()
                before(g2a, k, vm, h, d)
            r0 = pl.multiple_of(me2[h] * sr, sr)
            v = (
                own[s, h, pl.ds(r0, sr), :] + r2b[s, h, 0].astype(f32) + r2b[s, h, 1].astype(f32)
            ).astype(bf16)
            fin[s, h] = v
            if vm:
                a = pl.multiple_of(
                    (core * SIDE + me1[h]) * up_rows + (k - first) * ROWS + h * ph + me2[h] * sr, sr
                )
                wv[0, pl.ds(a, sr), :] = v
            for d in range(2):
                g2a(k, vm, h, d).start()
            if not vm:
                fin_local(k, h).start()

    def S5(k, vm):
        for h, d in hd:
            g2a(k, vm, h, d).wait_recv()
            before(g2b, k, vm, h, d)
            g2b(k, vm, h, d).start()
        if not vm:
            for h in range(2):
                fin_local(k, h).wait()

    def S6(k, vm):
        for h, d in hd:
            g2b(k, vm, h, d).wait_recv()
        for p in range(2):
            for h, d in hd:
                before(g1a, k, vm, h, d, p)
                g1a(k, vm, h, d, p).start()

    def S7(k, vm):
        for h, d in hd:
            g1a(k, vm, h, d, 0).wait_recv()
            before(g1b, k, vm, h, d)
            g1b(k, vm, h, d).start()
        for h in range(2):
            before(dd, k, vm, h, 0)
            dd(k, vm, h, 0).start()

    def S8(k, vm):
        for h, d in hd:
            g1a(k, vm, h, d, 1).wait_recv()
        for h in range(2):
            for o in (1, 3):
                before(dd, k, vm, h, o)
                dd(k, vm, h, o).start()
        for h, d in hd:
            g1b(k, vm, h, d).wait_recv()
        for h in range(2):
            before(dd, k, vm, h, 2)
            dd(k, vm, h, 2).start()

    ho = [(h, o) for h in range(2) for o in range(4)]

    def back(p):
        return pltpu.make_async_copy(
            y_hbm.at[:, pl.ds(p * pc, pc)], wv.at[1, pl.ds(p * up_rows, up_rows), :], back_sem.at[p]
        )

    reduce = dict(S1=S1, S2=S2, S3=S3)
    gather = dict(S4=S4, S5=S5, S6=S6, S7=S7, S8=S8)

    @pl.loop(0, N_STEPS)
    def _(step):
        t, i = step // STEPS, lax.rem(step, STEPS)

        @pl.when((t < chunks) & (i < nt))
        def _():
            gate_up(t, i)

        @pl.when((t < chunks) & (i >= nt))
        def _():
            down(t, i - nt)

        for name in ("S2", "S4", "S1", "S3", "S5", "S6", "S7", "S8"):
            at = POS[name]
            assert len(at) == chunks
            hit = step == at[0]
            k = jnp.int32(0)
            for p in at[1:]:
                hit = hit | (step == p)
            for p in at:
                k = k + jnp.where(step > p, 1, 0)
            if name in reduce:
                @pl.when(hit)
                def _():
                    reduce[name](k)
            else:
                @pl.when(hit & (k < first))
                def _():
                    gather[name](k, False)

                @pl.when(hit & (k >= first))
                def _():
                    gather[name](k, True)

        @pl.when(step == POS_BACK)
        def _():
            @pl.loop(0, first)
            def _(k):
                for h, o in ho:
                    dd(k, False, h, o).wait_recv()

            for p in range(2 * SIDE):
                back(p).start()

    for p in range(2 * SIDE):
        back(p).wait()
    for k in range(first, chunks):
        for h, o in ho:
            dd(k, True, h, o).wait_recv()
    for n in range(D_SLOTS):
        d_copy(last, 0, n).wait_send()
    for h, d in hd:
        for f in (c1a, c2a, c2b):
            f(last, h, d).wait_send()
        for p in range(2):
            c1b(last, h, d, p).wait_send()
    for k in (last - 1, last):
        for h, d in hd:
            for f in (g2a, g2b, g1b):
                f(k, True, h, d).wait_send()
            for p in range(2):
                g1a(k, True, h, d, p).wait_send()
        for h, o in ho:
            dd(k, True, h, o).wait_send()


def _write(v_ref, y_ref, sem):
    pieces = y_ref.shape[1] // v_ref.shape[2]
    rows = v_ref.shape[1] // pieces
    copies = []
    for g in range(2):
        for p in range(pieces):
            src = v_ref.at[1 - g, pl.ds(p * rows, rows), :]
            dst = y_ref.at[pl.ds(g * rows, rows), pl.ds(p * v_ref.shape[2], v_ref.shape[2])]
            copies.append(pltpu.make_async_copy(src, dst, sem.at[g, p]))
    for c in copies:
        c.start()
    for c in copies:
        c.wait()


def solution(mesh):
    def step(x, w_gate, w_up, w_down):
        rows, depth = x.shape
        hidden = w_gate.shape[1]
        cols = w_down.shape[1]
        chunks = rows // ROWS
        pc = cols // 2 // SIDE
        ph = ROWS // 2
        sr = ph // SIDE
        assert mesh.shape["tp"] == 2 * SIDE * SIDE
        assert depth == cols and SIDE * rows == depth and hidden == 4 * NT == pc
        bf16, f32 = jnp.bfloat16, jnp.float32
        dma = pltpu.SemaphoreType.DMA
        V = pltpu.VMEM
        _, v = pl.pallas_call(
            _kernel,
            out_shape=(
                jax.ShapeDtypeStruct((rows // 2, cols), bf16),
                pltpu.VMEM((2, depth, pc), bf16),
            ),
            in_specs=[pl.BlockSpec(memory_space=pl.ANY)] * 4,
            out_specs=(
                pl.BlockSpec(memory_space=pl.ANY),
                pl.BlockSpec(memory_space=pltpu.VMEM),
            ),
            scratch_shapes=[
                V((ROWS, depth), bf16),
                V((ROWS, hidden), bf16),
                V((WD_SLOTS, hidden, pc), bf16),
                V((SIDE, ROWS, pc), f32),
                V((D_SLOTS, ROWS, pc), bf16),
                V((2, SIDE, ROWS, pc), bf16),
                V((2, 2, ph // 2, pc), bf16),
                V((2, 2, 2, ph // 2, pc), bf16),
                V((2, 2, ph, pc), bf16),
                V((2, 2, 2, ph, pc), bf16),
                V((2, 2, ph, pc), f32),
                V((2, 2, sr // 2, pc), bf16),
                V((2, 2, 2, sr // 2, pc), bf16),
                V((2, 2, sr, pc), bf16),
                V((2, 2, 2, sr, pc), bf16),
                V((2, 2, sr, pc), bf16),
                dma, dma((hidden // NT, 2)), dma((WD_SLOTS,)), dma((D_SLOTS,)), dma((2, SIDE)),
                dma((2, 2)), dma((2, 2, 2)), dma((2, 2, 2)), dma((2, 2, 2, 2)),
                dma((2, 2)), dma((2, 2, 2)), dma((2, 2)), dma((2, 2, 2)),
                dma((2, 2)),
                dma((2, 2, 2)), dma((chunks, 2, 2)), dma((2, 2, 2)), dma((chunks, 2, 2)),
                dma((2, 2, 2, 2)), dma((chunks, 2, 2, 2)), dma((2, 2, 2)), dma((chunks, 2, 2)),
                dma((2, 2, SIDE)), dma((chunks, 2, SIDE)),
                pltpu.SemaphoreType.REGULAR, dma((2 * SIDE,)),
            ],
            compiler_params=pltpu.CompilerParams(
                collective_id=0, has_side_effects=True, vmem_limit_bytes=67043328 - 4 * depth * pc
            ),
            cost_estimate=pl.CostEstimate(
                flops=6 * rows * depth * hidden, bytes_accessed=0, transcendentals=0
            ),
        )(x, w_gate, w_up, w_down)

        return pl.pallas_call(
            _write,
            out_shape=jax.ShapeDtypeStruct((rows, cols), bf16),
            in_specs=[pl.BlockSpec(memory_space=pltpu.VMEM)],
            out_specs=pl.BlockSpec(memory_space=pl.ANY),
            scratch_shapes=[dma((2, 2 * SIDE))],
            compiler_params=pltpu.CompilerParams(vmem_limit_bytes=2**22),
        )(pltpu.with_memory_space_constraint(v, pltpu.VMEM))

    return jax.shard_map(
        step,
        mesh=mesh,
        in_specs=(P("dp", None), P(None, "tp"), P(None, "tp"), P("tp", None)),
        out_specs=P("dp", None),
        check_vma=False,
    )
```
